32 devices in a mesh: gx: 4 (over z), gy: 4 (over y, x), gz: 2 (over core).
Axes of the slice: x: 2, y: 2, z: 4, core: 2. Of those that a mesh axis runs over, the one named last changes fastest.
Arguments:
- test_vectors: float32 [8, 64, 64, 2048], P(None, 'gx', 'gy', 'gz'), as said below
- aniso: int32 [3, 2], replicated, may hold values from 2 to 4
Outputs:
- basis: float32 [8, 64, 64, 2048], P(None, 'gx', 'gy', 'gz')
- coarse_basis: float32 [8, 32, 32, 1024], P(None, 'gx', 'gy', 'gz')
The draws below stay inside these ranges and needn't reach their ends.
Inputs may be any that keep to these rules, and one draw needn't show every extreme that they name: `test_vectors`: positive and negative values; every test vector is linearly independent of the others.
All inputs are finite; a program needn't handle non-finite values.
Results may differ from the reference program's by a relative error of at most 0.00029.
Values sent between devices are 32-bit elements; how exact they have to be, the bound alone decides.
A program may use at most 384 MiB of HBM per device.

```python
import jax
import jax.numpy as jnp
from jax import lax

K = 8
SWEEPS = 3
NX = 64
NY = 64
NZ = 2048


def draw_test_vectors(key, part):
    key_noise = jax.random.fold_in(key, 11)
    key_cells = jax.random.fold_in(key, 12)
    key_vectors = jax.random.fold_in(key, 13)
    key_blocks = jax.random.fold_in(key, 15)
    full_shape = (K, NX, NY, NZ)
    grid_shape = (1, NX, NY, NZ)
    index_x = lax.broadcasted_iota(jnp.float32, grid_shape, 1) / NX
    index_y = lax.broadcasted_iota(jnp.float32, grid_shape, 2) / NY
    index_z = lax.broadcasted_iota(jnp.float32, grid_shape, 3) / NZ
    position = (index_x + index_y + index_z) / 3.0
    values = jax.random.normal(key_noise, full_shape, jnp.float32)
    envelope = jnp.exp(jnp.log(3.0) * position)
    cell_scale = jnp.exp(jax.random.uniform(key_cells, grid_shape, jnp.float32, 0.0, jnp.log(10.0)))
    vector_scale = jnp.exp(jax.random.uniform(key_vectors, (K, 1, 1, 1), jnp.float32, 0.0, jnp.log(10.0)))
    block_table = jnp.exp(jax.random.uniform(key_blocks, (K, 2, 2, 2), jnp.float32, 0.0, jnp.log(10.0)))
    block_x = lax.broadcasted_iota(jnp.int32, (NX, 1, 1), 0) * 2 // NX
    block_y = lax.broadcasted_iota(jnp.int32, (1, NY, 1), 1) * 2 // NY
    block_z = lax.broadcasted_iota(jnp.int32, (1, 1, NZ), 2) * 2 // NZ
    block_scale = block_table[:, block_x, block_y, block_z]
    return values * cell_scale * vector_scale * block_scale * envelope


def set_ends(array, key, least, top_value):
    longest = array.shape.index(max(array.shape))
    spots = []
    for shift in (0, 1):
        where = [jax.random.randint(jax.random.fold_in(key, axis), (), 0, length) for axis, length in enumerate(array.shape)]
        where[longest] = (where[longest] + shift) % array.shape[longest]
        spots.append(tuple(where))
    return array.at[spots[0]].set(least).at[spots[1]].set(top_value)


def setup_inputs(seed: int = 0) -> dict:
    splits = jax.random.split(jax.random.key(seed), 3)
    return {
        "test_vectors": draw_test_vectors(jax.random.fold_in(splits[2], 71), 0),
        "aniso": set_ends(jax.random.randint(splits[1], (3, 2), 2, 5), jax.random.fold_in(splits[1], 1), 2, 4).astype(jnp.int32),
    }


omega_weight = 2.0 / 3.0

def jacobi_sweep(fields, coefficients, scaled):
    padded = jnp.pad(fields, ((0, 0), (1, 1), (1, 1), (1, 1)))
    center = padded[:, 1:-1, 1:-1, 1:-1]
    beside = coefficients[0] * (padded[:, 2:, 1:-1, 1:-1] + padded[:, :-2, 1:-1, 1:-1])
    beside = beside + coefficients[1] * (padded[:, 1:-1, 2:, 1:-1] + padded[:, 1:-1, :-2, 1:-1])
    beside = beside + coefficients[2] * (padded[:, 1:-1, 1:-1, 2:] + padded[:, 1:-1, 1:-1, :-2])
    return (1.0 - omega_weight) * center + scaled * beside

def orthonormal(gram_total, data):
    lower_factor = jnp.linalg.cholesky(gram_total)
    eye_matrix = jnp.eye(gram_total.shape[0], dtype=gram_total.dtype)
    inverse = jax.scipy.linalg.solve_triangular(lower_factor, eye_matrix, lower=True)
    return jnp.einsum('kl,lxyz->kxyz', inverse, data, precision=lax.Precision.HIGHEST)

def reference(test_vectors, aniso):
    coefficients = aniso[:, 0].astype(jnp.float32) / aniso[:, 1].astype(jnp.float32)
    scaled = omega_weight / (2.0 * (coefficients[0] + coefficients[1] + coefficients[2]))
    fields = test_vectors
    for sweep_index in range(SWEEPS):
        fields = jacobi_sweep(fields, coefficients, scaled)
    flattened = fields.reshape(K, -1)
    cell_count = NX * NY * NZ
    gram_total = jnp.dot(flattened, flattened.T, precision=lax.Precision.HIGHEST) / cell_count
    coarse = fields.reshape(K, NX // 2, 2, NY // 2, 2, NZ // 2, 2).mean(axis=(2, 4, 6))
    coarse_flat = coarse.reshape(K, -1)
    coarse_gram = jnp.dot(coarse_flat, coarse_flat.T, precision=lax.Precision.HIGHEST) / (cell_count // 8)
    return (orthonormal(gram_total, fields), orthonormal(coarse_gram, coarse))
```

```python
import functools

import jax
import jax.numpy as jnp
from jax import lax
from jax.experimental import pallas as pl
from jax.experimental.pallas import tpu as pltpu
from jax.sharding import PartitionSpec as P

SWEEPS = 3
OMEGA = 2.0 / 3.0
MESH = pl.DeviceIdType.MESH
HIGHEST = lax.Precision.HIGHEST
AXES = ("gx", "gy", "gz")


def inverse_factor(gram):
    k = gram.shape[0]
    row = lax.broadcasted_iota(jnp.int32, gram.shape, 0)
    lane = lax.broadcasted_iota(jnp.int32, gram.shape, 1)
    m = jnp.where(lane < k, gram, 0.0) + jnp.where(lane == row + k, 1.0, 0.0)
    scale = jnp.zeros(gram.shape, jnp.float32)
    for j in range(k):
        pivot_row = m[j : j + 1, :]
        pivot = pivot_row[:, j : j + 1]
        column = m[:, j : j + 1]
        scale = jnp.where(row == j, pivot, scale)
        m = m - jnp.where(row > j, (column / pivot) * pivot_row, 0.0)
    return m / jnp.sqrt(scale)


def relax_kernel(
    sizes, cells, aniso_ref, v_ref, f_out, c_out, inv_ref, cinv_ref,
    f0, f1, f2, ys, yh, zh, cs, gp, cgp, *rest,
):
    gbs, (in_sem, out_sem, c_sem, send_sem, recv_sem, gsend, grecv) = rest[:3], rest[3:]
    vectors, rows_x, rows_y, rows_z = v_ref.shape
    me = {axis: lax.axis_index(axis) for axis in AXES}
    bufs = (f0, f1, f2)

    def load(k):
        return pltpu.make_async_copy(v_ref.at[k], f0.at[k, pl.ds(1, rows_x)], in_sem.at[k])

    for k in range(vectors):
        load(k).start()

    def halo(r, k, axis, side):
        f = bufs[r]
        if axis == 0:
            src = f.at[k, rows_x if side == 0 else 1]
            dst = f.at[k, 0 if side == 0 else rows_x + 1]
        elif axis == 1:
            src = ys.at[r, side, k]
            dst = yh.at[r, side, k]
        else:
            src = f.at[k, pl.ds(1, rows_x), :, pl.ds(rows_z - 128 if side == 0 else 0, 128)]
            dst = zh.at[r, side, k]
        name = AXES[axis]
        target = me[name] + 1 if side == 0 else me[name] - 1
        return pltpu.make_async_remote_copy(
            src_ref=src,
            dst_ref=dst,
            send_sem=send_sem.at[r, k, axis, side],
            recv_sem=recv_sem.at[r, k, axis, side],
            device_id={name: target},
            device_id_type=MESH,
        )

    def sends_to(axis, side):
        name = AXES[axis]
        return me[name] < sizes[axis] - 1 if side == 0 else me[name] > 0

    def gets_from(axis, side):
        name = AXES[axis]
        return me[name] > 0 if side == 0 else me[name] < sizes[axis] - 1

    barrier = pltpu.get_barrier_semaphore()
    peers = 0
    for axis, name in enumerate(AXES):
        for d in range(1, sizes[axis]):
            pl.semaphore_signal(
                barrier, inc=1,
                device_id={name: lax.rem(me[name] + d, sizes[axis])}, device_id_type=MESH,
            )
            peers += 1

    for axis in range(2):
        for side in range(2):
            @pl.when(jnp.logical_not(gets_from(axis, side)))
            def _():
                def clear(k, _):
                    for r in range(SWEEPS):
                        zero = jnp.zeros((rows_y if axis == 0 else rows_x, rows_z), jnp.float32)
                        if axis == 0:
                            bufs[r][k, 0 if side == 0 else rows_x + 1] = zero
                        else:
                            yh[r, side, k] = zero
                    return 0

                lax.fori_loop(0, vectors, clear, 0)

    def quotient(d):
        top = jnp.full((8, 128), aniso_ref[d, 0], jnp.int32).astype(jnp.float32)
        return top / jnp.full((8, 128), aniso_ref[d, 1], jnp.int32).astype(jnp.float32)

    coefficients = [quotient(d) for d in range(3)]
    scaled = OMEGA / (2.0 * (coefficients[0] + coefficients[1] + coefficients[2]))
    reps = (rows_y // 8, rows_z // 128)
    w = [jnp.tile(c * scaled, reps) for c in coefficients]

    pl.semaphore_wait(barrier, peers)

    def pack(r, k):
        f = bufs[r]
        for x in range(rows_x):
            ys[r, 0, k, pl.ds(x, 1), :] = f[k, x + 1, pl.ds(rows_y - 1, 1), :]
            ys[r, 1, k, pl.ds(x, 1), :] = f[k, x + 1, pl.ds(0, 1), :]

    def send(r, k):
        for axis in range(3):
            for side in range(2):
                @pl.when(sends_to(axis, side))
                def _():
                    halo(r, k, axis, side).start()

    def receive(r, k):
        for axis in range(3):
            for side in range(2):
                @pl.when(gets_from(axis, side))
                def _():
                    halo(r, k, axis, side).wait_recv()

    def finish_send(r, k):
        for axis in range(3):
            for side in range(2):
                @pl.when(sends_to(axis, side))
                def _():
                    halo(r, k, axis, side).wait_send()

    def first(k, _):
        load(k).wait()
        pack(0, k)
        send(0, k)
        return 0

    lax.fori_loop(0, vectors, first, 0)

    lane = lax.broadcasted_iota(jnp.int32, (rows_y, 128), 1)
    row = lax.broadcasted_iota(jnp.int32, (rows_y, rows_z), 0)
    use_high = jnp.logical_and(lane < 64, gets_from(2, 1))
    use_low = jnp.logical_and(lane >= 64, gets_from(2, 0))

    def sweep(r, k):
        f, out = bufs[r], bufs[(r + 1) % 3]

        def body(x, _):
            c = f[k, x + 1]
            side_z = jnp.where(use_high, zh[r, 1, k, x], jnp.where(use_low, zh[r, 0, k, x], 0.0))
            wide = jnp.concatenate([c, side_z], axis=1)
            width = rows_z + 128
            beside_z = pltpu.roll(wide, 1, 1)[:, :rows_z] + pltpu.roll(wide, width - 1, 1)[:, :rows_z]
            below = jnp.where(row == 0, yh[r, 0, k, pl.ds(x, 1), :], pltpu.roll(c, 1, 0))
            above = jnp.where(
                row == rows_y - 1, yh[r, 1, k, pl.ds(x, 1), :], pltpu.roll(c, rows_y - 1, 0)
            )
            total = w[0] * (f[k, x] + f[k, x + 2]) + w[1] * (below + above) + w[2] * beside_z
            out[k, x + 1] = (1.0 - OMEGA) * c + total
            return 0

        lax.fori_loop(0, rows_x, body, 0)

    for r in range(SWEEPS - 1):
        def step(k, _):
            receive(r, k)
            sweep(r, k)
            pack(r + 1, k)
            send(r + 1, k)
            return 0

        lax.fori_loop(0, vectors, step, 0)

    pair_z = jnp.where(
        lax.broadcasted_iota(jnp.int32, (256, 128), 0) // 2
        == lax.broadcasted_iota(jnp.int32, (256, 128), 1),
        0.125, 0.0,
    )
    half = rows_x // 2 * rows_y
    pair_y = jnp.where(
        lax.broadcasted_iota(jnp.int32, (half // 2, half), 0)
        == lax.broadcasted_iota(jnp.int32, (half // 2, half), 1) // 2,
        1.0, 0.0,
    )

    def tile_sum(product):
        parts = [
            product[i : i + 8, j : j + 128]
            for i in range(0, product.shape[0], 8)
            for j in range(0, product.shape[1], 128)
        ]
        while len(parts) > 1:
            parts = [sum(parts[i : i + 2]) for i in range(0, len(parts), 2)]
        return parts[0]

    def out_copy(k):
        return pltpu.make_async_copy(f0.at[k, pl.ds(1, rows_x)], f_out.at[k], out_sem.at[k])

    def coarse_copy(k):
        return pltpu.make_async_copy(cs.at[k], c_out.at[k], c_sem.at[k])

    def last(k, _):
        receive(SWEEPS - 1, k)
        finish_send(0, k)
        sweep(SWEEPS - 1, k)
        out_copy(k).start()
        for j in range(rows_z // 256):
            block = jnp.concatenate(
                [
                    f0[k, 2 * x + 1, :, pl.ds(256 * j, 256)] + f0[k, 2 * x + 2, :, pl.ds(256 * j, 256)]
                    for x in range(rows_x // 2)
                ],
                axis=0,
            )
            thin = jnp.dot(block, pair_z, precision=HIGHEST, preferred_element_type=jnp.float32)
            mean = jnp.dot(pair_y, thin, precision=HIGHEST, preferred_element_type=jnp.float32)
            cs[k, :, :, pl.ds(128 * j, 128)] = mean.reshape(rows_x // 2, rows_y // 2, 128)
        coarse_copy(k).start()

        def pair(l, _):
            def add(x, acc):
                return acc + tile_sum(f0[k, x + 1] * f0[l, x + 1])

            acc = lax.fori_loop(0, rows_x, add, jnp.zeros((8, 128), jnp.float32))
            line = jnp.sum(acc, axis=0, keepdims=True)
            gp[l, pl.ds(k, 1), :] = line
            gp[k, pl.ds(l, 1), :] = line
            acc = jnp.zeros((8, 128), jnp.float32)
            for x in range(rows_x // 2):
                acc = acc + tile_sum(cs[k, x] * cs[l, x])
            line = jnp.sum(acc, axis=0, keepdims=True)
            cgp[l, pl.ds(k, 1), :] = line
            cgp[k, pl.ds(l, 1), :] = line
            return 0

        lax.fori_loop(0, k + 1, pair, 0)
        return 0

    lax.fori_loop(0, vectors, last, 0)

    lane8 = lax.broadcasted_iota(jnp.int32, (vectors, 128), 1)
    gram = jnp.zeros((vectors, 128), jnp.float32)
    for l in range(vectors):
        gram = jnp.where(lane8 == l, jnp.sum(gp[l], axis=1, keepdims=True), gram)
        gram = jnp.where(lane8 == l + 64, jnp.sum(cgp[l], axis=1, keepdims=True), gram)

    for axis, name in enumerate(AXES):
        gb = gbs[axis]
        here = me[name]
        gb[here] = gram
        copies = [
            pltpu.make_async_remote_copy(
                src_ref=gb.at[here],
                dst_ref=gb.at[here],
                send_sem=gsend.at[axis, d],
                recv_sem=grecv.at[axis, d],
                device_id={name: lax.rem(here + d, sizes[axis])},
                device_id_type=MESH,
            )
            for d in range(1, sizes[axis])
        ]
        for copy in copies:
            copy.start()
        for d in range(1, sizes[axis]):
            source = lax.rem(here + sizes[axis] - d, sizes[axis])
            pltpu.make_async_remote_copy(
                src_ref=gb.at[source],
                dst_ref=gb.at[source],
                send_sem=gsend.at[axis, d],
                recv_sem=grecv.at[axis, d],
                device_id={name: lax.rem(here + d, sizes[axis])},
                device_id_type=MESH,
            ).wait_recv()
        for copy in copies:
            copy.wait_send()
        gram = gb[0]
        for i in range(1, sizes[axis]):
            gram = gram + gb[i]

    inv_ref[...] = inverse_factor(gram / cells)
    cinv_ref[...] = inverse_factor(pltpu.roll(gram, 64, 1) / (cells // 8))

    def drain(k, _):
        for r in range(1, SWEEPS):
            finish_send(r, k)
        out_copy(k).wait()
        coarse_copy(k).wait()
        return 0

    lax.fori_loop(0, vectors, drain, 0)


def apply_kernel(inv_ref, cinv_ref, f_ref, c_ref, b_ref, cb_ref):
    k_count = f_ref.shape[0]

    def combine(factor, src, dst, columns):
        data = [src[l, 0, :, columns] for l in range(k_count)]
        for k in range(k_count):
            total = factor[k, k_count] * data[0]
            for l in range(1, k + 1):
                total = total + factor[k, k_count + l] * data[l]
            dst[k, 0, :, columns] = total

    for j in range(0, f_ref.shape[3], 128):
        combine(inv_ref, f_ref, b_ref, pl.ds(j, 128))
    for j in range(0, c_ref.shape[3], 128):
        combine(cinv_ref, c_ref, cb_ref, pl.ds(j, 128))


def local(sizes, test_vectors, aniso):
    vectors, rows_x, rows_y, rows_z = test_vectors.shape
    coarse_shape = (vectors, rows_x // 2, rows_y // 2, rows_z // 2)
    cells = rows_x * rows_y * rows_z * sizes[0] * sizes[1] * sizes[2]
    f32 = jnp.float32
    field = pltpu.VMEM((vectors, rows_x + 2, rows_y, rows_z), f32)
    most = max(sizes)
    small = jax.ShapeDtypeStruct((vectors, 128), f32)
    fields, coarse, inv, cinv = pl.pallas_call(
        functools.partial(relax_kernel, sizes, cells),
        out_shape=(
            jax.ShapeDtypeStruct(test_vectors.shape, f32),
            jax.ShapeDtypeStruct(coarse_shape, f32),
            small,
            small,
        ),
        in_specs=[pl.BlockSpec(memory_space=pltpu.SMEM), pl.BlockSpec(memory_space=pl.ANY)],
        out_specs=(
            pl.BlockSpec(memory_space=pl.ANY),
            pl.BlockSpec(memory_space=pl.ANY),
            pl.BlockSpec(memory_space=pltpu.VMEM),
            pl.BlockSpec(memory_space=pltpu.VMEM),
        ),
        scratch_shapes=[
            field,
            field,
            field,
            pltpu.VMEM((SWEEPS, 2, vectors, rows_x, rows_z), f32),
            pltpu.VMEM((SWEEPS, 2, vectors, rows_x, rows_z), f32),
            pltpu.VMEM((SWEEPS, 2, vectors, rows_x, rows_y, 128), f32),
            pltpu.VMEM(coarse_shape, f32),
            pltpu.VMEM((vectors, vectors, 128), f32),
            pltpu.VMEM((vectors, vectors, 128), f32),
            *[pltpu.VMEM((n, vectors, 128), f32) for n in sizes],
            pltpu.SemaphoreType.DMA((vectors,)),
            pltpu.SemaphoreType.DMA((vectors,)),
            pltpu.SemaphoreType.DMA((vectors,)),
            pltpu.SemaphoreType.DMA((SWEEPS, vectors, 3, 2)),
            pltpu.SemaphoreType.DMA((SWEEPS, vectors, 3, 2)),
            pltpu.SemaphoreType.DMA((3, most)),
            pltpu.SemaphoreType.DMA((3, most)),
        ],
        compiler_params=pltpu.CompilerParams(
            collective_id=0, has_side_effects=True, vmem_limit_bytes=60 * 2**20
        ),
    )(aniso, test_vectors)
    block = pl.BlockSpec((vectors, 1, rows_y, rows_z), lambda i: (0, i, 0, 0))
    coarse_block = pl.BlockSpec(
        (vectors, 1, rows_y // 2, rows_z // 4), lambda i: (0, i // 2, 0, i % 2)
    )
    factor = pl.BlockSpec(memory_space=pltpu.SMEM)
    return pl.pallas_call(
        apply_kernel,
        grid=(rows_x,),
        out_shape=(
            jax.ShapeDtypeStruct(test_vectors.shape, f32),
            jax.ShapeDtypeStruct(coarse_shape, f32),
        ),
        in_specs=[factor, factor, block, coarse_block],
        out_specs=(block, coarse_block),
    )(inv, cinv, fields, coarse)


def solution(mesh):
    sizes = tuple(mesh.shape[axis] for axis in AXES)
    spec = P(None, *AXES)
    return jax.shard_map(
        functools.partial(local, sizes),
        mesh=mesh,
        in_specs=(spec, P()),
        out_specs=(spec, spec),
        check_vma=False,
    )
```

```python
import functools

import jax
import jax.numpy as jnp
from jax import lax
from jax.experimental import pallas as pl
from jax.experimental.pallas import tpu as pltpu
from jax.sharding import PartitionSpec as P

SWEEPS = 3
SWEEP_UNROLL = 16
OMEGA = 2.0 / 3.0
MESH = pl.DeviceIdType.MESH
HIGHEST = lax.Precision.HIGHEST
AXES = ("gx", "gy", "gz")


def inverse_factor(gram):
    k = gram.shape[0]
    row = lax.broadcasted_iota(jnp.int32, gram.shape, 0)
    lane = lax.broadcasted_iota(jnp.int32, gram.shape, 1)
    m = jnp.where(lane < k, gram, 0.0) + jnp.where(lane == row + k, 1.0, 0.0)
    scale = jnp.zeros(gram.shape, jnp.float32)
    for j in range(k):
        pivot_row = m[j : j + 1, :]
        pivot = pivot_row[:, j : j + 1]
        column = m[:, j : j + 1]
        scale = jnp.where(row == j, pivot, scale)
        m = m - jnp.where(row > j, (column / pivot) * pivot_row, 0.0)
    return m / jnp.sqrt(scale)


def relax_kernel(
    sizes, cells, relayed, aniso_ref, v_ref, f_out, c_out, inv_ref, cinv_ref,
    f0, f1, f2, ys, yh, zh, rb, thin, cs, gp, cgp, gb, *rest,
):
    in_sem, out_sem, c_sem, send_sem, recv_sem, gsend, grecv, *relay_sems = rest
    up_send, up_recv, down_send, down_recv = relay_sems
    vectors, rows_x, rows_y, rows_z = v_ref.shape
    me = {axis: lax.axis_index(axis) for axis in AXES}
    bufs = (f0, f1, f2)

    def load(k):
        return pltpu.make_async_copy(v_ref.at[k], f0.at[k, pl.ds(1, rows_x)], in_sem.at[k])

    for k in range(vectors):
        load(k).start()

    def halo(r, k, axis, side):
        f = bufs[r]
        if axis == 0:
            src = f.at[k, rows_x if side == 0 else 1]
            dst = f.at[k, 0 if side == 0 else rows_x + 1]
        elif axis == 1:
            src = ys.at[r, side, k]
            dst = yh.at[r, side, k]
        else:
            src = f.at[k, pl.ds(1, rows_x), :, pl.ds(rows_z - 128 if side == 0 else 0, 128)]
            dst = zh.at[r, side, k]
        name = AXES[axis]
        target = me[name] + 1 if side == 0 else me[name] - 1
        return pltpu.make_async_remote_copy(
            src_ref=src,
            dst_ref=dst,
            send_sem=send_sem.at[r, k, axis, side],
            recv_sem=recv_sem.at[r, k, axis, side],
            device_id={name: target},
            device_id_type=MESH,
        )

    def gets_from(axis, side):
        name = AXES[axis]
        return me[name] > 0 if side == 0 else me[name] < sizes[axis] - 1

    def direct_to(axis, side):
        name = AXES[axis]
        there = me[name] < sizes[axis] - 1 if side == 0 else me[name] > 0
        if relayed and axis == 1:
            there = jnp.logical_and(there, me[name] != (1 if side == 0 else 2))
        return there

    def direct_from(axis, side):
        there = gets_from(axis, side)
        if relayed and axis == 1:
            there = jnp.logical_and(there, me["gy"] != (2 if side == 0 else 1))
        return there

    part = rows_x // 2
    ways = ((0, 1, 2), (1, 2, 1))
    relays = ((0, 0), (1, 3))

    def to_relay(r, k, side, half, by):
        return pltpu.make_async_remote_copy(
            src_ref=ys.at[r, side, k, pl.ds(half * part, part)],
            dst_ref=rb.at[r, side, k],
            send_sem=up_send.at[r, k, half],
            recv_sem=up_recv.at[r, k, side],
            device_id={"gy": by},
            device_id_type=MESH,
        )

    def from_relay(r, k, side, half, target):
        return pltpu.make_async_remote_copy(
            src_ref=rb.at[r, side, k],
            dst_ref=yh.at[r, side, k, pl.ds(half * part, part)],
            send_sem=down_send.at[r, k, side],
            recv_sem=down_recv.at[r, k, half],
            device_id={"gy": target},
            device_id_type=MESH,
        )

    def forward(r, k):
        for half, by in relays if relayed else ():
            @pl.when(me["gy"] == by)
            def _():
                for side, source, target in ways:
                    to_relay(r, k, side, half, by).wait_recv()
                    from_relay(r, k, side, half, target).start()

    barrier = pltpu.get_barrier_semaphore()
    devices = sizes[0] * sizes[1] * sizes[2]
    here = (me["gx"] * sizes[1] + me["gy"]) * sizes[2] + me["gz"]

    def place(index):
        return {
            "gx": index // (sizes[1] * sizes[2]),
            "gy": lax.rem(index // sizes[2], sizes[1]),
            "gz": lax.rem(index, sizes[2]),
        }

    def greet(d, _):
        other = place(lax.rem(here + d, devices))
        pl.semaphore_signal(barrier, inc=1, device_id=other, device_id_type=MESH)
        return 0

    lax.fori_loop(1, devices, greet, 0)

    for axis in range(2):
        for side in range(2):
            @pl.when(jnp.logical_not(gets_from(axis, side)))
            def _():
                def clear(k, _):
                    for r in range(SWEEPS):
                        zero = jnp.zeros((rows_y if axis == 0 else rows_x, rows_z), jnp.float32)
                        if axis == 0:
                            bufs[r][k, 0 if side == 0 else rows_x + 1] = zero
                        else:
                            yh[r, side, k] = zero
                    return 0

                lax.fori_loop(0, vectors, clear, 0)

    def quotient(d):
        top = jnp.full((8, 128), aniso_ref[0, d], jnp.int32).astype(jnp.float32)
        return top / jnp.full((8, 128), aniso_ref[1, d], jnp.int32).astype(jnp.float32)

    coefficients = [quotient(d) for d in range(3)]
    scaled = OMEGA / (2.0 * (coefficients[0] + coefficients[1] + coefficients[2]))
    reps = (rows_y // 8, rows_z // 128)
    w = [jnp.tile(c * scaled, reps) for c in coefficients]

    pl.semaphore_wait(barrier, devices - 1)

    def pack(r, k):
        f = bufs[r]
        for x in range(rows_x):
            ys[r, 0, k, pl.ds(x, 1), :] = f[k, x + 1, pl.ds(rows_y - 1, 1), :]
            ys[r, 1, k, pl.ds(x, 1), :] = f[k, x + 1, pl.ds(0, 1), :]

    def send(r, k):
        for side, source, target in ways if relayed else ():
            @pl.when(me["gy"] == source)
            def _():
                for half, by in relays:
                    to_relay(r, k, side, half, by).start()
        for axis in range(3):
            for side in range(2):
                @pl.when(direct_to(axis, side))
                def _():
                    halo(r, k, axis, side).start()

    def receive(r, k):
        forward(r, k)
        for axis in range(3):
            for side in range(2):
                @pl.when(direct_from(axis, side))
                def _():
                    halo(r, k, axis, side).wait_recv()
        for side, source, target in ways if relayed else ():
            @pl.when(me["gy"] == target)
            def _():
                for half, by in relays:
                    from_relay(r, k, side, half, target).wait_recv()

    def finish_send(r, k):
        for axis in range(3):
            for side in range(2):
                @pl.when(direct_to(axis, side))
                def _():
                    halo(r, k, axis, side).wait_send()
        for side, source, target in ways if relayed else ():
            @pl.when(me["gy"] == source)
            def _():
                for half, by in relays:
                    to_relay(r, k, side, half, by).wait_send()
        for half, by in relays if relayed else ():
            @pl.when(me["gy"] == by)
            def _():
                for side, source, target in ways:
                    from_relay(r, k, side, half, target).wait_send()

    def first(k, _):
        load(k).wait()
        pack(0, k)
        send(0, k)
        return 0

    lax.fori_loop(0, vectors, first, 0)

    lane = lax.broadcasted_iota(jnp.int32, (rows_y, 128), 1)
    row = lax.broadcasted_iota(jnp.int32, (rows_y, rows_z), 0)
    use_high = jnp.logical_and(lane < 64, gets_from(2, 1))
    use_low = jnp.logical_and(lane >= 64, gets_from(2, 0))

    def sweep(r, k):
        f, out = bufs[r], bufs[(r + 1) % 3]

        def body(x, _):
            c = f[k, x + 1]
            side_z = jnp.where(use_high, zh[r, 1, k, x], jnp.where(use_low, zh[r, 0, k, x], 0.0))
            wide = jnp.concatenate([c, side_z], axis=1)
            width = rows_z + 128
            beside_z = pltpu.roll(wide, 1, 1)[:, :rows_z] + pltpu.roll(wide, width - 1, 1)[:, :rows_z]
            below = jnp.where(row == 0, yh[r, 0, k, pl.ds(x, 1), :], pltpu.roll(c, 1, 0))
            above = jnp.where(
                row == rows_y - 1, yh[r, 1, k, pl.ds(x, 1), :], pltpu.roll(c, rows_y - 1, 0)
            )
            total = w[0] * (f[k, x] + f[k, x + 2]) + w[1] * (below + above) + w[2] * beside_z
            out[k, x + 1] = (1.0 - OMEGA) * c + total
            return 0

        lax.fori_loop(0, rows_x, body, 0, unroll=SWEEP_UNROLL)

    for r in range(SWEEPS - 1):
        def step(k, _):
            receive(r, k)
            sweep(r, k)
            pack(r + 1, k)
            send(r + 1, k)
            return 0

        lax.fori_loop(0, vectors, step, 0)

    pair_z = jnp.where(
        lax.broadcasted_iota(jnp.int32, (256, 128), 0) // 2
        == lax.broadcasted_iota(jnp.int32, (256, 128), 1),
        0.125, 0.0,
    ).astype(jnp.bfloat16)
    half = rows_x // 2 * rows_y
    def tile_sum(product):
        parts = [
            product[i : i + 8, j : j + 128]
            for i in range(0, product.shape[0], 8)
            for j in range(0, product.shape[1], 128)
        ]
        while len(parts) > 1:
            parts = [sum(parts[i : i + 2]) for i in range(0, len(parts), 2)]
        return parts[0]

    def out_copy(k):
        return pltpu.make_async_copy(f0.at[k, pl.ds(1, rows_x)], f_out.at[k], out_sem.at[k])

    def coarse_copy(k):
        return pltpu.make_async_copy(cs.at[k], c_out.at[k], c_sem.at[k])

    def last(k, _):
        receive(SWEEPS - 1, k)
        finish_send(0, k)
        sweep(SWEEPS - 1, k)
        out_copy(k).start()
        block = jnp.concatenate(
            [
                f0[k, 2 * x + 1, :, pl.ds(256 * j, 256)] + f0[k, 2 * x + 2, :, pl.ds(256 * j, 256)]
                for j in range(rows_z // 256)
                for x in range(rows_x // 2)
            ],
            axis=0,
        )
        top = block.astype(jnp.bfloat16)
        left = block - top.astype(jnp.float32)
        middle = left.astype(jnp.bfloat16)
        low = (left - middle.astype(jnp.float32)).astype(jnp.bfloat16)
        thin[...] = sum(
            jnp.dot(piece, pair_z, preferred_element_type=jnp.float32)
            for piece in (low, middle, top)
        )
        for j in range(rows_z // 256):
            even = thin[pl.ds(half * j, half // 2, stride=2), :]
            odd = thin[pl.ds(half * j + 1, half // 2, stride=2), :]
            cs[k, :, :, pl.ds(128 * j, 128)] = (even + odd).reshape(rows_x // 2, rows_y // 2, 128)
        coarse_copy(k).start()

        def pair(l, _):
            def add(x, acc):
                return acc + tile_sum(f0[k, x + 1] * f0[l, x + 1])

            acc = lax.fori_loop(0, rows_x, add, jnp.zeros((8, 128), jnp.float32), unroll=4)
            line = jnp.sum(acc, axis=0, keepdims=True)
            gp[l, pl.ds(k, 1), :] = line
            gp[k, pl.ds(l, 1), :] = line
            acc = jnp.zeros((8, 128), jnp.float32)
            for x in range(rows_x // 2):
                acc = acc + tile_sum(cs[k, x] * cs[l, x])
            line = jnp.sum(acc, axis=0, keepdims=True)
            cgp[l, pl.ds(k, 1), :] = line
            cgp[k, pl.ds(l, 1), :] = line
            return 0

        lax.fori_loop(0, k + 1, pair, 0)
        return 0

    lax.fori_loop(0, vectors, last, 0)

    lane8 = lax.broadcasted_iota(jnp.int32, (vectors, 128), 1)
    gram = jnp.zeros((vectors, 128), jnp.float32)
    for l in range(vectors):
        gram = jnp.where(lane8 == l, jnp.sum(gp[l], axis=1, keepdims=True), gram)
        gram = jnp.where(lane8 == l + 64, jnp.sum(cgp[l], axis=1, keepdims=True), gram)

    line = gram[0:1]
    for k in range(1, vectors):
        line = line + pltpu.roll(gram[k : k + 1], vectors * k, 1)
    gb[here] = line

    def share(d, slot):
        return pltpu.make_async_remote_copy(
            src_ref=gb.at[slot],
            dst_ref=gb.at[slot],
            send_sem=gsend.at[d],
            recv_sem=grecv.at[d],
            device_id=place(lax.rem(here + d, devices)),
            device_id_type=MESH,
        )

    def share_start(d, _):
        share(d, here).start()
        return 0

    def share_recv(d, _):
        share(d, lax.rem(here + devices - d, devices)).wait_recv()
        return 0

    def share_sent(d, _):
        share(d, here).wait_send()
        return 0

    lax.fori_loop(1, devices, share_start, 0)
    lax.fori_loop(1, devices, share_recv, 0)
    line = jnp.sum(gb[...], axis=0)
    row8 = lax.broadcasted_iota(jnp.int32, (vectors, 128), 0)
    gram = jnp.broadcast_to(line, (vectors, 128))
    for k in range(1, vectors):
        gram = jnp.where(row8 == k, pltpu.roll(line, 128 - vectors * k, 1), gram)

    inv_ref[...] = inverse_factor(gram / cells)
    cinv_ref[...] = inverse_factor(pltpu.roll(gram, 64, 1) / (cells // 8))

    def drain(k, _):
        for r in range(1, SWEEPS):
            finish_send(r, k)
        out_copy(k).wait()
        coarse_copy(k).wait()
        return 0

    lax.fori_loop(0, vectors, drain, 0)
    lax.fori_loop(1, devices, share_sent, 0)


def apply_kernel(inv_ref, cinv_ref, f_ref, c_ref, b_ref, cb_ref):
    k_count = f_ref.shape[0]

    def combine(factor, src, dst, x, columns):
        data = [src[l, x, :, columns] for l in range(k_count)]
        for k in range(k_count):
            total = factor[k, k_count] * data[0]
            for l in range(1, k + 1):
                total = total + factor[k, k_count + l] * data[l]
            dst[k, x, :, columns] = total

    for x in range(f_ref.shape[1]):
        for j in range(0, f_ref.shape[3], 128):
            combine(inv_ref, f_ref, b_ref, x, pl.ds(j, 128))
    for x in range(c_ref.shape[1]):
        for j in range(0, c_ref.shape[3], 128):
            combine(cinv_ref, c_ref, cb_ref, x, pl.ds(j, 128))


def local(sizes, test_vectors, aniso):
    vectors, rows_x, rows_y, rows_z = test_vectors.shape
    coarse_shape = (vectors, rows_x // 2, rows_y // 2, rows_z // 2)
    cells = rows_x * rows_y * rows_z * sizes[0] * sizes[1] * sizes[2]
    f32 = jnp.float32
    field = pltpu.VMEM((vectors, rows_x + 2, rows_y, rows_z), f32)
    devices = sizes[0] * sizes[1] * sizes[2]
    relayed = sizes[1] == 4 and sizes[2] == 2
    small = jax.ShapeDtypeStruct((vectors, 128), f32)
    fields, coarse, inv, cinv = pl.pallas_call(
        functools.partial(relax_kernel, sizes, cells, relayed),
        out_shape=(
            jax.ShapeDtypeStruct(test_vectors.shape, f32),
            jax.ShapeDtypeStruct(coarse_shape, f32),
            small,
            small,
        ),
        in_specs=[pl.BlockSpec(memory_space=pltpu.SMEM), pl.BlockSpec(memory_space=pl.ANY)],
        out_specs=(
            pl.BlockSpec(memory_space=pl.ANY),
            pl.BlockSpec(memory_space=pl.ANY),
            pl.BlockSpec(memory_space=pltpu.VMEM),
            pl.BlockSpec(memory_space=pltpu.VMEM),
        ),
        scratch_shapes=[
            field,
            field,
            field,
            pltpu.VMEM((SWEEPS, 2, vectors, rows_x, rows_z), f32),
            pltpu.VMEM((SWEEPS, 2, vectors, rows_x, rows_z), f32),
            pltpu.VMEM((SWEEPS, 2, vectors, rows_x, rows_y, 128), f32),
            pltpu.VMEM((SWEEPS, 2, vectors, rows_x // 2, rows_z), f32),
            pltpu.VMEM((rows_x * rows_y * rows_z // 512, 128), f32),
            pltpu.VMEM(coarse_shape, f32),
            pltpu.VMEM((vectors, vectors, 128), f32),
            pltpu.VMEM((vectors, vectors, 128), f32),
            pltpu.VMEM((devices, 1, 128), f32),
            pltpu.SemaphoreType.DMA((vectors,)),
            pltpu.SemaphoreType.DMA((vectors,)),
            pltpu.SemaphoreType.DMA((vectors,)),
            pltpu.SemaphoreType.DMA((SWEEPS, vectors, 3, 2)),
            pltpu.SemaphoreType.DMA((SWEEPS, vectors, 3, 2)),
            pltpu.SemaphoreType.DMA((devices,)),
            pltpu.SemaphoreType.DMA((devices,)),
            *[pltpu.SemaphoreType.DMA((SWEEPS, vectors, 2))] * 4,
        ],
        compiler_params=pltpu.CompilerParams(
            collective_id=0, has_side_effects=True, vmem_limit_bytes=47 * 2**20
        ),
    )(aniso.T, test_vectors)
    block = pl.BlockSpec((vectors, 2, rows_y, rows_z), lambda i: (0, i, 0, 0))
    coarse_block = pl.BlockSpec((vectors, 1, rows_y // 2, rows_z // 2), lambda i: (0, i, 0, 0))
    factor = pl.BlockSpec(memory_space=pltpu.SMEM)
    return pl.pallas_call(
        apply_kernel,
        grid=(rows_x // 2,),
        out_shape=(
            jax.ShapeDtypeStruct(test_vectors.shape, f32),
            jax.ShapeDtypeStruct(coarse_shape, f32),
        ),
        in_specs=[factor, factor, block, coarse_block],
        out_specs=(block, coarse_block),
        compiler_params=pltpu.CompilerParams(vmem_limit_bytes=16 * 2**20),
    )(inv, cinv, fields, coarse)


def solution(mesh):
    sizes = tuple(mesh.shape[axis] for axis in AXES)
    spec = P(None, *AXES)
    return jax.shard_map(
        functools.partial(local, sizes),
        mesh=mesh,
        in_specs=(spec, P()),
        out_specs=(spec, spec),
        check_vma=False,
    )
```

```python
import functools

import jax
import jax.numpy as jnp
from jax import lax
from jax.experimental import pallas as pl
from jax.experimental.pallas import tpu as pltpu
from jax.sharding import PartitionSpec as P

SWEEPS = 3
SWEEP_UNROLL = 16
OMEGA = 2.0 / 3.0
MESH = pl.DeviceIdType.MESH
HIGHEST = lax.Precision.HIGHEST
AXES = ("gx", "gy", "gz")


def inverse_factor(gram):
    k = gram.shape[0]
    row = lax.broadcasted_iota(jnp.int32, gram.shape, 0)
    lane = lax.broadcasted_iota(jnp.int32, gram.shape, 1)
    m = jnp.where(lane < k, gram, 0.0) + jnp.where(lane == row + k, 1.0, 0.0)
    scale = jnp.zeros(gram.shape, jnp.float32)
    for j in range(k):
        pivot_row = m[j : j + 1, :]
        pivot = pivot_row[:, j : j + 1]
        column = m[:, j : j + 1]
        scale = jnp.where(row == j, pivot, scale)
        m = m - jnp.where(row > j, (column / pivot) * pivot_row, 0.0)
    return m / jnp.sqrt(scale)


def relax_kernel(
    sizes, cells, relayed, aniso_ref, v_ref, f_out, c_out, inv_ref, cinv_ref,
    f0, f1, f2, ys, yh, zh, rb, thin, cs, gp, cgp, gb, *rest,
):
    in_sem, out_sem, c_sem, send_sem, recv_sem, gsend, grecv, *relay_sems = rest
    up_send, up_recv, down_send, down_recv = relay_sems
    vectors, rows_x, rows_y, rows_z = v_ref.shape
    me = {axis: lax.axis_index(axis) for axis in AXES}
    bufs = (f0, f1, f2)

    def load(k):
        return pltpu.make_async_copy(v_ref.at[k], f0.at[k, pl.ds(1, rows_x)], in_sem.at[k])

    for k in range(vectors):
        load(k).start()

    def halo(r, k, axis, side):
        f = bufs[r]
        if axis == 0:
            src = f.at[k, rows_x if side == 0 else 1]
            dst = f.at[k, 0 if side == 0 else rows_x + 1]
        elif axis == 1:
            src = ys.at[r, side, k]
            dst = yh.at[r, side, k]
        else:
            src = f.at[k, pl.ds(1, rows_x), :, pl.ds(rows_z - 128 if side == 0 else 0, 128)]
            dst = zh.at[r, side, k]
        name = AXES[axis]
        target = me[name] + 1 if side == 0 else me[name] - 1
        return pltpu.make_async_remote_copy(
            src_ref=src,
            dst_ref=dst,
            send_sem=send_sem.at[r, k, axis, side],
            recv_sem=recv_sem.at[r, k, axis, side],
            device_id={name: target},
            device_id_type=MESH,
        )

    def gets_from(axis, side):
        name = AXES[axis]
        return me[name] > 0 if side == 0 else me[name] < sizes[axis] - 1

    def direct_to(axis, side):
        name = AXES[axis]
        there = me[name] < sizes[axis] - 1 if side == 0 else me[name] > 0
        if relayed and axis == 1:
            there = jnp.logical_and(there, me[name] != (1 if side == 0 else 2))
        return there

    def direct_from(axis, side):
        there = gets_from(axis, side)
        if relayed and axis == 1:
            there = jnp.logical_and(there, me["gy"] != (2 if side == 0 else 1))
        return there

    part = rows_x // 2
    ways = ((0, 1, 2), (1, 2, 1))
    relays = ((0, 0), (1, 3))

    def to_relay(r, k, side, half, by):
        return pltpu.make_async_remote_copy(
            src_ref=ys.at[r, side, k, pl.ds(half * part, part)],
            dst_ref=rb.at[r, side, k],
            send_sem=up_send.at[r, k, half],
            recv_sem=up_recv.at[r, k, side],
            device_id={"gy": by},
            device_id_type=MESH,
        )

    def from_relay(r, k, side, half, target):
        return pltpu.make_async_remote_copy(
            src_ref=rb.at[r, side, k],
            dst_ref=yh.at[r, side, k, pl.ds(half * part, part)],
            send_sem=down_send.at[r, k, side],
            recv_sem=down_recv.at[r, k, half],
            device_id={"gy": target},
            device_id_type=MESH,
        )

    def forward(r, k):
        for half, by in relays if relayed else ():
            @pl.when(me["gy"] == by)
            def _():
                for side, source, target in ways:
                    to_relay(r, k, side, half, by).wait_recv()
                    from_relay(r, k, side, half, target).start()

    barrier = pltpu.get_barrier_semaphore()
    devices = sizes[0] * sizes[1] * sizes[2]
    here = (me["gx"] * sizes[1] + me["gy"]) * sizes[2] + me["gz"]

    def place(index):
        return {
            "gx": index // (sizes[1] * sizes[2]),
            "gy": lax.rem(index // sizes[2], sizes[1]),
            "gz": lax.rem(index, sizes[2]),
        }

    def greet(d, _):
        other = place(lax.rem(here + d, devices))
        pl.semaphore_signal(barrier, inc=1, device_id=other, device_id_type=MESH)
        return 0

    lax.fori_loop(1, devices, greet, 0)

    for axis in range(2):
        for side in range(2):
            @pl.when(jnp.logical_not(gets_from(axis, side)))
            def _():
                def clear(k, _):
                    for r in range(SWEEPS):
                        zero = jnp.zeros((rows_y if axis == 0 else rows_x, rows_z), jnp.float32)
                        if axis == 0:
                            bufs[r][k, 0 if side == 0 else rows_x + 1] = zero
                        else:
                            yh[r, side, k] = zero
                    return 0

                lax.fori_loop(0, vectors, clear, 0)

    def quotient(d):
        top = jnp.full((8, 128), aniso_ref[0, d], jnp.int32).astype(jnp.float32)
        return top / jnp.full((8, 128), aniso_ref[1, d], jnp.int32).astype(jnp.float32)

    coefficients = [quotient(d) for d in range(3)]
    scaled = OMEGA / (2.0 * (coefficients[0] + coefficients[1] + coefficients[2]))
    reps = (rows_y // 8, rows_z // 128)
    w = [jnp.tile(c * scaled, reps) for c in coefficients]

    pl.semaphore_wait(barrier, devices - 1)

    def pack(r, k):
        f = bufs[r]
        for x in range(rows_x):
            ys[r, 0, k, pl.ds(x, 1), :] = f[k, x + 1, pl.ds(rows_y - 1, 1), :]
            ys[r, 1, k, pl.ds(x, 1), :] = f[k, x + 1, pl.ds(0, 1), :]

    def send(r, k):
        for side, source, target in ways if relayed else ():
            @pl.when(me["gy"] == source)
            def _():
                for half, by in relays:
                    to_relay(r, k, side, half, by).start()
        for axis in range(3):
            for side in range(2):
                @pl.when(direct_to(axis, side))
                def _():
                    halo(r, k, axis, side).start()

    def receive(r, k):
        forward(r, k)
        for axis in range(3):
            for side in range(2):
                @pl.when(direct_from(axis, side))
                def _():
                    halo(r, k, axis, side).wait_recv()
        for side, source, target in ways if relayed else ():
            @pl.when(me["gy"] == target)
            def _():
                for half, by in relays:
                    from_relay(r, k, side, half, target).wait_recv()

    def finish_send(r, k):
        for axis in range(3):
            for side in range(2):
                @pl.when(direct_to(axis, side))
                def _():
                    halo(r, k, axis, side).wait_send()
        for side, source, target in ways if relayed else ():
            @pl.when(me["gy"] == source)
            def _():
                for half, by in relays:
                    to_relay(r, k, side, half, by).wait_send()
        for half, by in relays if relayed else ():
            @pl.when(me["gy"] == by)
            def _():
                for side, source, target in ways:
                    from_relay(r, k, side, half, target).wait_send()

    def first(k, _):
        load(k).wait()
        pack(0, k)
        send(0, k)
        return 0

    lax.fori_loop(0, vectors, first, 0)

    lane = lax.broadcasted_iota(jnp.int32, (rows_y, 128), 1)
    row = lax.broadcasted_iota(jnp.int32, (rows_y, rows_z), 0)
    use_high = jnp.logical_and(lane < 64, gets_from(2, 1))
    use_low = jnp.logical_and(lane >= 64, gets_from(2, 0))

    def sweep(r, k):
        f, out = bufs[r], bufs[(r + 1) % 3]

        def body(x, _):
            c = f[k, x + 1]
            side_z = jnp.where(use_high, zh[r, 1, k, x], jnp.where(use_low, zh[r, 0, k, x], 0.0))
            wide = jnp.concatenate([c, side_z], axis=1)
            width = rows_z + 128
            beside_z = pltpu.roll(wide, 1, 1)[:, :rows_z] + pltpu.roll(wide, width - 1, 1)[:, :rows_z]
            below = jnp.where(row == 0, yh[r, 0, k, pl.ds(x, 1), :], pltpu.roll(c, 1, 0))
            above = jnp.where(
                row == rows_y - 1, yh[r, 1, k, pl.ds(x, 1), :], pltpu.roll(c, rows_y - 1, 0)
            )
            total = w[0] * (f[k, x] + f[k, x + 2]) + w[1] * (below + above) + w[2] * beside_z
            out[k, x + 1] = (1.0 - OMEGA) * c + total
            return 0

        lax.fori_loop(0, rows_x, body, 0, unroll=SWEEP_UNROLL)

    for r in range(SWEEPS - 1):
        def step(k, _):
            receive(r, k)
            sweep(r, k)
            pack(r + 1, k)
            send(r + 1, k)
            return 0

        lax.fori_loop(0, vectors, step, 0)

    pair_z = jnp.where(
        lax.broadcasted_iota(jnp.int32, (256, 128), 0) // 2
        == lax.broadcasted_iota(jnp.int32, (256, 128), 1),
        0.125, 0.0,
    ).astype(jnp.bfloat16)
    half = rows_x // 2 * rows_y
    def tile_sum(product):
        parts = [
            product[i : i + 8, j : j + 128]
            for i in range(0, product.shape[0], 8)
            for j in range(0, product.shape[1], 128)
        ]
        while len(parts) > 1:
            parts = [sum(parts[i : i + 2]) for i in range(0, len(parts), 2)]
        return parts[0]

    def out_copy(k):
        return pltpu.make_async_copy(f0.at[k, pl.ds(1, rows_x)], f_out.at[k], out_sem.at[k])

    def coarse_copy(k):
        return pltpu.make_async_copy(cs.at[k], c_out.at[k], c_sem.at[k])

    def last(k, _):
        receive(SWEEPS - 1, k)
        finish_send(0, k)
        sweep(SWEEPS - 1, k)
        out_copy(k).start()
        block = jnp.concatenate(
            [
                f0[k, 2 * x + 1, :, pl.ds(256 * j, 256)] + f0[k, 2 * x + 2, :, pl.ds(256 * j, 256)]
                for j in range(rows_z // 256)
                for x in range(rows_x // 2)
            ],
            axis=0,
        )
        top = block.astype(jnp.bfloat16)
        left = block - top.astype(jnp.float32)
        middle = left.astype(jnp.bfloat16)
        low = (left - middle.astype(jnp.float32)).astype(jnp.bfloat16)
        thin[...] = sum(
            jnp.dot(piece, pair_z, preferred_element_type=jnp.float32)
            for piece in (low, middle, top)
        )
        for j in range(rows_z // 256):
            even = thin[pl.ds(half * j, half // 2, stride=2), :]
            odd = thin[pl.ds(half * j + 1, half // 2, stride=2), :]
            cs[k, :, :, pl.ds(128 * j, 128)] = (even + odd).reshape(rows_x // 2, rows_y // 2, 128)
        coarse_copy(k).start()

        def pair(l, _):
            def add(x, acc):
                return acc + tile_sum(f0[k, x + 1] * f0[l, x + 1])

            acc = lax.fori_loop(0, rows_x, add, jnp.zeros((8, 128), jnp.float32), unroll=4)
            line = jnp.sum(acc, axis=0, keepdims=True)
            gp[l, pl.ds(k, 1), :] = line
            gp[k, pl.ds(l, 1), :] = line
            acc = jnp.zeros((8, 128), jnp.float32)
            for x in range(rows_x // 2):
                acc = acc + tile_sum(cs[k, x] * cs[l, x])
            line = jnp.sum(acc, axis=0, keepdims=True)
            cgp[l, pl.ds(k, 1), :] = line
            cgp[k, pl.ds(l, 1), :] = line
            return 0

        lax.fori_loop(0, k + 1, pair, 0)
        return 0

    lax.fori_loop(0, vectors, last, 0)

    lane8 = lax.broadcasted_iota(jnp.int32, (vectors, 128), 1)
    gram = jnp.zeros((vectors, 128), jnp.float32)
    for l in range(vectors):
        gram = jnp.where(lane8 == l, jnp.sum(gp[l], axis=1, keepdims=True), gram)
        gram = jnp.where(lane8 == l + 64, jnp.sum(cgp[l], axis=1, keepdims=True), gram)

    line = gram[0:1]
    for k in range(1, vectors):
        line = line + pltpu.roll(gram[k : k + 1], vectors * k, 1)
    gb[here] = line

    def share(d, slot):
        return pltpu.make_async_remote_copy(
            src_ref=gb.at[slot],
            dst_ref=gb.at[slot],
            send_sem=gsend.at[d],
            recv_sem=grecv.at[d],
            device_id=place(lax.rem(here + d, devices)),
            device_id_type=MESH,
        )

    def share_start(d, _):
        share(d, here).start()
        return 0

    def share_recv(d, _):
        share(d, lax.rem(here + devices - d, devices)).wait_recv()
        return 0

    def share_sent(d, _):
        share(d, here).wait_send()
        return 0

    lax.fori_loop(1, devices, share_start, 0)
    lax.fori_loop(1, devices, share_recv, 0)
    line = jnp.sum(gb[...], axis=0)
    row8 = lax.broadcasted_iota(jnp.int32, (vectors, 128), 0)
    gram = jnp.broadcast_to(line, (vectors, 128))
    for k in range(1, vectors):
        gram = jnp.where(row8 == k, pltpu.roll(line, 128 - vectors * k, 1), gram)

    inv_ref[...] = inverse_factor(gram / cells)
    cinv_ref[...] = inverse_factor(pltpu.roll(gram, 64, 1) / (cells // 8))

    def drain(k, _):
        for r in range(1, SWEEPS):
            finish_send(r, k)
        out_copy(k).wait()
        coarse_copy(k).wait()
        return 0

    lax.fori_loop(0, vectors, drain, 0)
    lax.fori_loop(1, devices, share_sent, 0)


def apply_kernel(inv_ref, cinv_ref, f_ref, c_ref, b_ref, cb_ref):
    k_count = f_ref.shape[0]

    def combine(factor, src, dst, x, columns):
        data = [src[l, x, :, columns] for l in range(k_count)]
        for k in range(k_count):
            total = factor[k, k_count] * data[0]
            for l in range(1, k + 1):
                total = total + factor[k, k_count + l] * data[l]
            dst[k, x, :, columns] = total

    for x in range(f_ref.shape[1]):
        for j in range(0, f_ref.shape[3], 256):
            combine(inv_ref, f_ref, b_ref, x, pl.ds(j, 256))
    for x in range(c_ref.shape[1]):
        for j in range(0, c_ref.shape[3], 128):
            combine(cinv_ref, c_ref, cb_ref, x, pl.ds(j, 128))


def local(sizes, test_vectors, aniso):
    vectors, rows_x, rows_y, rows_z = test_vectors.shape
    coarse_shape = (vectors, rows_x // 2, rows_y // 2, rows_z // 2)
    cells = rows_x * rows_y * rows_z * sizes[0] * sizes[1] * sizes[2]
    f32 = jnp.float32
    field = pltpu.VMEM((vectors, rows_x + 2, rows_y, rows_z), f32)
    devices = sizes[0] * sizes[1] * sizes[2]
    relayed = sizes[1] == 4 and sizes[2] == 2
    small = jax.ShapeDtypeStruct((vectors, 128), f32)
    fields, coarse, inv, cinv = pl.pallas_call(
        functools.partial(relax_kernel, sizes, cells, relayed),
        out_shape=(
            jax.ShapeDtypeStruct(test_vectors.shape, f32),
            jax.ShapeDtypeStruct(coarse_shape, f32),
            small,
            small,
        ),
        in_specs=[pl.BlockSpec(memory_space=pltpu.SMEM), pl.BlockSpec(memory_space=pl.ANY)],
        out_specs=(
            pl.BlockSpec(memory_space=pl.ANY),
            pl.BlockSpec(memory_space=pl.ANY),
            pl.BlockSpec(memory_space=pltpu.VMEM),
            pl.BlockSpec(memory_space=pltpu.VMEM),
        ),
        scratch_shapes=[
            field,
            field,
            field,
            pltpu.VMEM((SWEEPS, 2, vectors, rows_x, rows_z), f32),
            pltpu.VMEM((SWEEPS, 2, vectors, rows_x, rows_z), f32),
            pltpu.VMEM((SWEEPS, 2, vectors, rows_x, rows_y, 128), f32),
            pltpu.VMEM((SWEEPS, 2, vectors, rows_x // 2, rows_z), f32),
            pltpu.VMEM((rows_x * rows_y * rows_z // 512, 128), f32),
            pltpu.VMEM(coarse_shape, f32),
            pltpu.VMEM((vectors, vectors, 128), f32),
            pltpu.VMEM((vectors, vectors, 128), f32),
            pltpu.VMEM((devices, 1, 128), f32),
            pltpu.SemaphoreType.DMA((vectors,)),
            pltpu.SemaphoreType.DMA((vectors,)),
            pltpu.SemaphoreType.DMA((vectors,)),
            pltpu.SemaphoreType.DMA((SWEEPS, vectors, 3, 2)),
            pltpu.SemaphoreType.DMA((SWEEPS, vectors, 3, 2)),
            pltpu.SemaphoreType.DMA((devices,)),
            pltpu.SemaphoreType.DMA((devices,)),
            *[pltpu.SemaphoreType.DMA((SWEEPS, vectors, 2))] * 4,
        ],
        compiler_params=pltpu.CompilerParams(
            collective_id=0, has_side_effects=True, vmem_limit_bytes=60 * 2**20
        ),
    )(aniso.T, test_vectors)
    block = pl.BlockSpec((vectors, 4, rows_y, rows_z), lambda i: (0, i, 0, 0))
    coarse_block = pl.BlockSpec((vectors, 2, rows_y // 2, rows_z // 2), lambda i: (0, i, 0, 0))
    factor = pl.BlockSpec(memory_space=pltpu.SMEM)
    return pl.pallas_call(
        apply_kernel,
        grid=(rows_x // 4,),
        out_shape=(
            jax.ShapeDtypeStruct(test_vectors.shape, f32),
            jax.ShapeDtypeStruct(coarse_shape, f32),
        ),
        in_specs=[factor, factor, block, coarse_block],
        out_specs=(block, coarse_block),
        compiler_params=pltpu.CompilerParams(vmem_limit_bytes=60 * 2**20),
    )(inv, cinv, fields, coarse)


def solution(mesh):
    sizes = tuple(mesh.shape[axis] for axis in AXES)
    spec = P(None, *AXES)
    return jax.shard_map(
        functools.partial(local, sizes),
        mesh=mesh,
        in_specs=(spec, P()),
        out_specs=(spec, spec),
        check_vma=False,
    )
```
